256 devices in a mesh: section: 8 (over z_hi, core), expert: 32 (over z_lo, x, y).
Axes of the slice: x: 4, y: 4, z: 8 (z_hi: 4, z_lo: 2; z = z_hi * 2 + z_lo), core: 2. Of those that a mesh axis runs over, the one named last changes fastest.
Arguments:
- act_in: bfloat16 [8, 4096, 7168], P('section', 'expert'), may hold values from -6 to 6
- cotangent: bfloat16 [8, 4096, 7168], P('section', 'expert'), may hold values from -6 to 6
- fwd_ids: int32 [8, 4096, 8], P('section', 'expert'), may hold values from 0 to 255, as said below
- fwd_gates: float32 [8, 4096, 8], P('section', 'expert'), may hold values from 0.05 to 0.8
- bwd_ids: int32 [8, 4096, 8], P('section', 'expert'), may hold values from 0 to 255, as said below
- bwd_gates: float32 [8, 4096, 8], P('section', 'expert'), may hold values from 0.05 to 0.8
- gate_w: bfloat16 [8, 7168, 4096], P('section', None, 'expert'), may hold values from -0.0625 to 0.0625
- up_w: bfloat16 [8, 7168, 4096], P('section', None, 'expert'), may hold values from -0.0625 to 0.0625
- down_w: bfloat16 [8, 4096, 7168], P('section', 'expert'), may hold values from -0.125 to 0.125
- gate_pre: bfloat16 [8, 320, 4096], P('section', None, 'expert'), may hold values from -6 to 6
- up_pre: bfloat16 [8, 320, 4096], P('section', None, 'expert'), may hold values from -6 to 6
Outputs:
- next_act: bfloat16 [8, 4096, 7168], P('section', 'expert')
- prev_grad: bfloat16 [8, 4096, 7168], P('section', 'expert')
- gate_grad: float32 [8, 4096, 8], P('section', 'expert')
The draws below stay inside these ranges and needn't reach their ends.
Inputs may be any that keep to these rules, and one draw needn't show every extreme that they name: `fwd_ids`: the 8 ids of a row differ. In each aligned block of 128 rows (the rows of one device) each id below 2 is named by at most 10 rows; in every section one such id is named by exactly 10 rows in every block. `bwd_ids`: as for fwd_ids.
All inputs are finite; a program needn't handle non-finite values.
Results may differ from the reference program's by a relative error of at most 0.012.
Values may be sent and summed in bfloat16 or wider, within the bound.
No kernel may reach another device: no remote copies, remote signals or barrier semaphores. Data moves between devices by JAX's collectives and lax.ppermute only.
A program may use at most 128 MiB of HBM per device.

```python
import math
import jax
import jax.numpy as jnp
from jax import lax

D = 7168
FF = 2048
ROUTED = 256
TOP = 8
TOK_DEV = 128
CAP = 10
SLICES = 16
FF_DEV = 128
EXPERTS = 2
SECTIONS = 8
TOKENS = 4096
SLOTS = 320


def route_draw(key):
    blocks = SECTIONS * (TOKENS // TOK_DEV)
    keys = [jax.random.fold_in(key, offset) for offset in range(5)]
    counts = jax.random.randint(keys[0], (blocks, EXPERTS), CAP // 2, CAP + 1)
    fullest = jax.random.randint(keys[1], (SECTIONS,), 0, EXPERTS)
    fullest_block = jnp.repeat(fullest, TOKENS // TOK_DEV)
    counts = jnp.where(jnp.arange(EXPERTS)[None, :] == fullest_block[:, None], CAP, counts)
    scores = jax.random.randint(keys[2], (blocks, EXPERTS, TOK_DEV), 0, 2 ** 20) * TOK_DEV + jnp.arange(TOK_DEV)
    order = jnp.argsort(jnp.argsort(scores, axis=-1), axis=-1)
    chosen = order < counts[:, :, None]
    others = jax.random.randint(keys[3], (blocks, TOK_DEV, ROUTED - EXPERTS), 0, 2 ** 20) * ROUTED + jnp.arange(ROUTED - EXPERTS)
    unused, picks = lax.top_k(others, TOP)
    ids = picks + EXPERTS
    slot_scores = jax.random.randint(keys[4], (blocks, TOK_DEV, TOP), 0, 2 ** 20) * TOP + jnp.arange(TOP)
    unused_two, places = lax.top_k(slot_scores, TOP)
    slot_iota = jnp.arange(TOP)
    for expert in range(EXPERTS):
        target = places[:, :, expert:expert + 1]
        put_here = (slot_iota[None, None, :] == target) & chosen[:, expert, :, None]
        ids = jnp.where(put_here, expert, ids)
    return ids.reshape(SECTIONS, TOKENS, TOP).astype(jnp.int32)


def draw_fwd_ids(key, part):
    return route_draw(jax.random.fold_in(key, 11))


def draw_bwd_ids(key, part):
    return route_draw(jax.random.fold_in(key, 23))


def block_scale(key, extent, pieces, least, high):
    def one(dim, shards_of):
        draws = jax.random.uniform(jax.random.fold_in(jax.random.fold_in(key, 6), dim), (shards_of,), jnp.float32, least / len(pieces), high / len(pieces))
        return jnp.repeat(jnp.exp(draws), extent[dim] // shards_of).reshape((-1,) + (1,) * (len(extent) - dim - 1))

    level = one(*pieces[0])
    for cut in pieces[1:]:
        level = level * one(*cut)
    return level


def scatter_about(key, shape, width, reach, shards=(), held_as=jnp.bfloat16):
    values = width * jax.random.normal(key, shape, jnp.float32)
    if shards:
        values = values * block_scale(key, shape, shards, -0.22, 0.18)
    return jnp.clip(values, -reach, reach).astype(held_as)


def setup_inputs(seed: int = 0) -> dict:
    streams_of = jax.random.split(jax.random.key(seed), 12)
    return {
        "act_in": scatter_about(streams_of[0], (SECTIONS, TOKENS, D), 1.0, 6.0, ((0, 8), (1, 32))),
        "cotangent": scatter_about(streams_of[1], (SECTIONS, TOKENS, D), 1.0, 6.0, ((0, 8), (1, 32))),
        "fwd_ids": draw_fwd_ids(jax.random.fold_in(streams_of[11], 71), 0),
        "fwd_gates": jnp.clip(jnp.exp(math.log(0.8) - 2.7725887 * jax.random.uniform(streams_of[3], (SECTIONS, TOKENS, TOP), jnp.float32) ** block_scale(streams_of[3], (SECTIONS, TOKENS, TOP), ((0, 8), (1, 32)), -0.2, 0.2)), 0.05, 0.8),
        "bwd_ids": draw_bwd_ids(jax.random.fold_in(streams_of[11], 71), 0),
        "bwd_gates": jnp.clip(jnp.exp(math.log(0.8) - 2.7725887 * jax.random.uniform(streams_of[5], (SECTIONS, TOKENS, TOP), jnp.float32) ** block_scale(streams_of[5], (SECTIONS, TOKENS, TOP), ((0, 8), (1, 32)), -0.2, 0.2)), 0.05, 0.8),
        "gate_w": scatter_about(streams_of[6], (SECTIONS, D, EXPERTS * FF), D ** -0.5, 0.0625, ((0, 8), (2, 32))),
        "up_w": scatter_about(streams_of[7], (SECTIONS, D, EXPERTS * FF), D ** -0.5, 0.0625, ((0, 8), (2, 32))),
        "down_w": scatter_about(streams_of[8], (SECTIONS, EXPERTS * FF, D), FF ** -0.5, 0.125, ((0, 8), (1, 32))),
        "gate_pre": scatter_about(streams_of[9], (SECTIONS, SLOTS, EXPERTS * FF), 1.0, 6.0, ((0, 8), (2, 32))),
        "up_pre": scatter_about(streams_of[10], (SECTIONS, SLOTS, EXPERTS * FF), 1.0, 6.0, ((0, 8), (2, 32))),
    }


def slots_of(ids, expert):
    matches = ids == expert
    routed = jnp.any(matches, axis=1)
    blocks = routed.reshape(-1, TOK_DEV).astype(jnp.int32)
    position = (jnp.cumsum(blocks, axis=1) - 1).reshape(-1)
    block_ids = jnp.arange(TOKENS, dtype=jnp.int32) // TOK_DEV
    slot = jnp.where(routed, block_ids * CAP + position, SLOTS).astype(jnp.int32)
    return matches, slot


def place_rows(tokens, slot):
    empty = jnp.zeros((SLOTS, tokens.shape[1]), tokens.dtype)
    return empty.at[slot].set(tokens, mode="drop")


def take_rows(table, slot):
    return jnp.take(table, jnp.minimum(slot, SLOTS - 1).astype(jnp.int32), axis=0)


def rounded_sum(parts):
    rounded = lax.optimization_barrier(parts.astype(jnp.bfloat16))
    return jnp.sum(rounded.astype(jnp.float32), axis=0)


def section_layer(tokens, grads, ids_f, gates_f, ids_b, gates_b, w_gate, w_up, w_down, pre_gate, pre_up):
    mixed = jnp.zeros((TOKENS, D), jnp.float32)
    input_grad = jnp.zeros((TOKENS, D), jnp.float32)
    gate_grad = jnp.zeros((TOKENS, TOP), jnp.float32)
    for expert in range(EXPERTS):
        lo_col = expert * FF
        wg_e = w_gate[:, lo_col:lo_col + FF]
        wu_e = w_up[:, lo_col:lo_col + FF]
        wd_e = w_down[lo_col:lo_col + FF]
        matches, slot = slots_of(ids_f, expert)
        weights = jnp.sum(jnp.where(matches, gates_f, 0.0), axis=1)
        rows = place_rows(tokens, slot)
        gate_act = jnp.dot(rows, wg_e, preferred_element_type=jnp.float32)
        up_act = jnp.dot(rows, wu_e, preferred_element_type=jnp.float32)
        hidden = (jax.nn.silu(gate_act) * up_act).astype(jnp.bfloat16)
        parts = jnp.einsum("rsf,sfd->srd", hidden.reshape(SLOTS, SLICES, FF_DEV).astype(jnp.float32),
                           wd_e.reshape(SLICES, FF_DEV, D).astype(jnp.float32))
        expert_out = rounded_sum(parts)
        mixed = mixed + weights[:, None] * take_rows(expert_out, slot)

        matches_b, slot_b = slots_of(ids_b, expert)
        weights_b = jnp.sum(jnp.where(matches_b, gates_b, 0.0), axis=1)
        grad_rows = place_rows(grads, slot_b)
        saved_gate = pre_gate[:, lo_col:lo_col + FF].astype(jnp.float32)
        saved_up = pre_up[:, lo_col:lo_col + FF].astype(jnp.float32)
        grad_hidden = jnp.dot(grad_rows, wd_e.T, preferred_element_type=jnp.float32)
        sigmoid_gate = jax.nn.sigmoid(saved_gate)
        activated = saved_gate * sigmoid_gate
        dot_parts = jnp.sum((grad_hidden * activated * saved_up).reshape(SLOTS, SLICES, FF_DEV), axis=2)
        expert_dot = rounded_sum(dot_parts.T)
        grad_gate_act = (grad_hidden * saved_up * sigmoid_gate * (1.0 + saved_gate * (1.0 - sigmoid_gate))).astype(jnp.bfloat16)
        grad_up_act = (grad_hidden * activated).astype(jnp.bfloat16)
        grad_parts = jnp.einsum("rsf,dsf->srd", grad_gate_act.reshape(SLOTS, SLICES, FF_DEV).astype(jnp.float32),
                                wg_e.reshape(D, SLICES, FF_DEV).astype(jnp.float32))
        grad_parts = grad_parts + jnp.einsum("rsf,dsf->srd", grad_up_act.reshape(SLOTS, SLICES, FF_DEV).astype(jnp.float32),
                                             wu_e.reshape(D, SLICES, FF_DEV).astype(jnp.float32))
        expert_grad = rounded_sum(grad_parts)
        input_grad = input_grad + weights_b[:, None] * take_rows(expert_grad, slot_b)
        gate_grad = gate_grad + jnp.where(matches_b, take_rows(expert_dot, slot_b)[:, None], 0.0)
    return mixed.astype(jnp.bfloat16), input_grad.astype(jnp.bfloat16), gate_grad


def reference(act_in, cotangent, fwd_ids, fwd_gates, bwd_ids, bwd_gates, gate_w, up_w, down_w, gate_pre, up_pre):
    outputs = []
    grads = []
    gate_grads = []
    for section in range(SECTIONS):
        mixed, input_grad, gate_grad = section_layer(act_in[section], cotangent[section], fwd_ids[section], fwd_gates[section],
                                                   bwd_ids[section], bwd_gates[section], gate_w[section], up_w[section],
                                                   down_w[section], gate_pre[section], up_pre[section])
        outputs.append(mixed)
        grads.append(input_grad)
        gate_grads.append(gate_grad)
    next_act = jnp.roll(jnp.stack(outputs), 1, axis=0)
    prev_grad = jnp.roll(jnp.stack(grads), -1, axis=0)
    return next_act, prev_grad, jnp.stack(gate_grads)
```

```python
import jax
import jax.numpy as jnp
from jax import lax
from jax.sharding import Mesh, PartitionSpec as P

CAP = 10
TOK = 128
D = 7168
HALF = D // 2
F = 128
ROWS = (16, 24)
UP = [(i, (i + 1) % 4) for i in range(4)]
DN = [(i, (i - 1) % 4) for i in range(4)]
OFFS = (0, -1, 1, 2)
f32 = jnp.float32
bf16 = jnp.bfloat16


def ring_gather(x, axis):
    left = lax.ppermute(x, axis, UP)
    right = lax.ppermute(x, axis, DN)
    h = x.shape[-1] // 2
    far_a = lax.ppermute(left[..., :h], axis, UP)
    far_b = lax.ppermute(right[..., h:], axis, DN)
    return [x, left, right, jnp.concatenate([far_a, far_b], -1)]


def ring_scatter(parts, axis):
    own, left, right, far = parts
    h = (own.shape[-1] // 256) * 128
    far_a = lax.ppermute(far[..., :h], axis, DN)
    far_b = lax.ppermute(far[..., h:], axis, UP)
    left = jnp.concatenate(
        [(left[..., :h].astype(f32) + far_a.astype(f32)).astype(bf16), left[..., h:]], -1
    )
    right = jnp.concatenate(
        [right[..., :h], (right[..., h:].astype(f32) + far_b.astype(f32)).astype(bf16)], -1
    )
    from_right = lax.ppermute(left, axis, DN)
    from_left = lax.ppermute(right, axis, UP)
    return (own.astype(f32) + from_right.astype(f32) + from_left.astype(f32)).astype(bf16)


def routing(ids, gates):
    expert_ids = jnp.arange(2, dtype=jnp.int32)
    matches = ids[None, :, :] == expert_ids[:, None, None]
    routed = jnp.any(matches, axis=2)
    weights = jnp.sum(jnp.where(matches, gates[None, :, :], 0.0), axis=2)
    position = jnp.cumsum(routed.astype(jnp.int32), axis=1) - 1
    slot_ids = jnp.arange(CAP, dtype=jnp.int32)
    placing = (position[:, None, :] == slot_ids[None, :, None]) & routed[:, None, :]
    return matches, placing.astype(f32), weights


def own_other(pair, z):
    own = jnp.where(z == 0, pair[0], pair[1])
    other = jnp.where(z == 0, pair[1], pair[0])
    return own, other


def slot_index(z, x, y):
    offs = jnp.array(OFFS, jnp.int32)
    block = ((x + offs) % 4)[None, :] * 4 + ((y + offs) % 4)[:, None]
    own = (z * 16 + block) * CAP
    other = ((1 - z) * 16 + block) * CAP
    far = jnp.full((4, 4, CAP), -1, jnp.int32)
    rank = jnp.arange(CAP, dtype=jnp.int32)
    first = jnp.concatenate([far, own[..., None] + rank[:6]], -1)
    second = jnp.concatenate([own[..., None] + rank[6:], far, other[..., None] + rank], -1)
    return first, second


def expert_rows(gathered_a, gathered_b, w1, w2, pre, is_fwd, lane):
    rows = is_fwd.shape[0]
    xa = jnp.stack(gathered_a).reshape(16 * rows, HALF)
    xb = jnp.stack(gathered_b).reshape(16 * rows, HALF)
    za = jnp.dot(xa, w1[:HALF], preferred_element_type=f32)
    zb = jnp.dot(xb, w1[HALF:], preferred_element_type=f32)
    zb = zb.reshape(4, 4, rows, 384).transpose(1, 0, 2, 3)
    z = za.reshape(4, 4, rows, 384) + zb
    fwd = is_fwd[None, None, :, None]
    hidden = jax.nn.silu(z[..., :F]) * z[..., F : 2 * F]
    g = pre[..., :F]
    u = pre[..., F:]
    grad_hidden = z[..., 2 * F :]
    s = jax.nn.sigmoid(g)
    activated = g * s
    dots = jnp.sum(grad_hidden * activated * u, axis=-1, keepdims=True)
    grad_gate = grad_hidden * u * s * (1.0 + g * (1.0 - s))
    grad_up = grad_hidden * activated
    h = jnp.concatenate(
        [
            jnp.where(fwd, hidden, 0.0),
            jnp.where(fwd, 0.0, grad_gate),
            jnp.where(fwd, 0.0, grad_up),
        ],
        -1,
    ).astype(bf16)
    h_t = h.transpose(1, 0, 2, 3)
    out_a = jnp.dot(h.reshape(16 * rows, 384), w2[:, :HALF], preferred_element_type=f32)
    out_b = jnp.dot(h_t.reshape(16 * rows, 384), w2[:, HALF:], preferred_element_type=f32)
    lanes = jnp.arange(128) == lane
    dots = jnp.where(lanes, jnp.where(fwd, 0.0, dots), 0.0).astype(bf16)
    out_a = out_a.astype(bf16).reshape(4, 4, rows, HALF)
    out_b = out_b.astype(bf16).reshape(4, 4, rows, HALF)
    out_b = jnp.concatenate([out_b, dots.transpose(1, 0, 2, 3)], -1)
    return out_a, out_b


def body(
    act_in, cotangent, fwd_ids, fwd_gates, bwd_ids, bwd_gates,
    gate_w, up_w, down_w, gate_pre, up_pre,
):
    z = lax.axis_index("z")
    x = lax.axis_index("x")
    y = lax.axis_index("y")
    matches_f, placing_f, weights_f = routing(fwd_ids[0], fwd_gates[0])
    matches_b, placing_b, weights_b = routing(bwd_ids[0], bwd_gates[0])
    own_f, other_f = own_other(placing_f, z)
    own_b, other_b = own_other(placing_b, z)
    none = jnp.zeros_like(own_f)
    pick_f = jnp.concatenate([own_f, none, other_f, none]).astype(bf16)
    pick_b = jnp.concatenate([none, own_b, none, other_b]).astype(bf16)
    rows = jnp.dot(pick_f, act_in[0], preferred_element_type=f32) + jnp.dot(
        pick_b, cotangent[0], preferred_element_type=f32
    )
    rows = rows.astype(bf16)
    first = rows[:16]
    swapped = lax.ppermute(rows[16:], "z", [(0, 1), (1, 0)])
    second = jnp.where(jnp.arange(24)[:, None] < 4, rows[16:], swapped)

    scale_f = lax.ppermute(
        (placing_f * weights_f[:, None, :]).reshape(2 * CAP, TOK), "section",
        [(i, (i + 1) % 8) for i in range(8)],
    )
    scale_b = lax.ppermute(
        (placing_b * weights_b[:, None, :]).reshape(2 * CAP, TOK), "section",
        [(i, (i - 1) % 8) for i in range(8)],
    )

    w1 = jnp.concatenate([gate_w[0], up_w[0], down_w[0].T], 1)
    w2 = jnp.concatenate([down_w[0], gate_w[0].T, up_w[0].T], 0)
    pre = jnp.concatenate([gate_pre[0], up_pre[0]], 1)
    slots = jnp.arange(pre.shape[0], dtype=jnp.int32)
    results = []
    for chunk, index, n in zip((first, second), slot_index(z, x, y), ROWS):
        pick = (index[..., None] == slots).astype(bf16)
        pre_rows = jnp.einsum("abrs,sf->abrf", pick, pre, preferred_element_type=f32)
        ga = ring_gather(jnp.stack(ring_gather(chunk[:, :HALF], "x")), "y")
        gb = ring_gather(jnp.stack(ring_gather(chunk[:, HALF:], "y")), "x")
        row = jnp.arange(n)
        is_fwd = row < CAP if n == 16 else (row >= 4) & (row < 14)
        oa, ob = expert_rows(ga, gb, w1, w2, pre_rows, is_fwd, x * 4 + y)
        ra = ring_scatter([oa[k] for k in range(4)], "y")
        rb = ring_scatter([ob[k] for k in range(4)], "x")
        ra = ring_scatter([ra[k] for k in range(4)], "x")
        rb = ring_scatter([rb[k] for k in range(4)], "y")
        results.append((ra, rb[:, :HALF], rb[:, HALF:]))
    (a0, b0, d0), (a1, b1, d1) = results

    def hop(a, b, step, flip):
        both = jnp.concatenate([a, b], 0)
        pairs = []
        for s in range(8):
            for zz in range(2):
                pairs.append((s * 2 + zz, (s + step) % 8 * 2 + (zz ^ flip)))
        out = lax.ppermute(both, ("section", "z"), pairs)
        return jnp.concatenate([out[:CAP], out[CAP:]], 1)

    fo = hop(a0[:10], b0[:10], 1, 0)
    bo = hop(jnp.concatenate([a0[10:], a1[:4]], 0), jnp.concatenate([b0[10:], b1[:4]], 0), -1, 0)
    fx = hop(a1[4:14], b1[4:14], 1, 1)
    bx = hop(a1[14:], b1[14:], -1, 1)

    def place(own, other, scale):
        r = jnp.where(z == 0, jnp.concatenate([own, other], 0), jnp.concatenate([other, own], 0))
        out = jnp.einsum("rt,rd->td", scale, r.astype(f32), precision=lax.Precision.HIGHEST)
        return out.astype(bf16)[None]

    next_act = place(fo, fx, scale_f)
    prev_grad = place(bo, bx, scale_b)

    dots0 = jnp.sum(d0.astype(f32), axis=1, keepdims=True)
    dots1 = jnp.sum(d1.astype(f32), axis=1, keepdims=True)
    dots_own = jnp.concatenate([dots0[10:], dots1[:4]], 0)
    dots_send = jnp.broadcast_to(dots1[14:], (CAP, 128))
    dots_other = lax.ppermute(dots_send, "z", [(0, 1), (1, 0)])[:, :1]
    dots = jnp.stack(
        [jnp.where(z == 0, dots_own, dots_other), jnp.where(z == 0, dots_other, dots_own)]
    )
    token_dots = jnp.sum(placing_b * dots, axis=1)
    gate_grad = jnp.sum(jnp.where(matches_b, token_dots[:, :, None], 0.0), axis=0)
    return next_act, prev_grad, gate_grad[None]


def solution(mesh):
    grid = Mesh(mesh.devices.reshape(8, 2, 4, 4), ("section", "z", "x", "y"))
    ex = ("z", "x", "y")
    tok = P("section", ex, None)
    col = P("section", None, ex)
    in_specs = (tok, tok, tok, tok, tok, tok, col, col, tok, col, col)
    return jax.shard_map(
        body, mesh=grid, in_specs=in_specs, out_specs=(tok, tok, tok), check_vma=False
    )
```

```python
import jax
import jax.numpy as jnp
from jax import lax
from jax.sharding import Mesh, PartitionSpec as P

CAP = 10
TOK = 128
D = 7168
F = 128
ROWS = 40
QUARTER = D // 4
SWAPS = (
    ("x", [(i, i ^ 1) for i in range(4)]),
    ("x", [(i, 3 - i) for i in range(4)]),
    ("y", [(i, i ^ 1) for i in range(4)]),
    ("y", [(i, 3 - i) for i in range(4)]),
)
GRAY = (0, 1, 3, 2)
f32 = jnp.float32
bf16 = jnp.bfloat16


def swap(v, d):
    axis, pairs = SWAPS[d]
    return lax.ppermute(v, axis, pairs)


def half(v, d, side):
    return lax.slice_in_dim(v, side, side + 1, axis=3 - d)


def routing(ids, gates):
    expert_ids = jnp.arange(2, dtype=jnp.int32)
    matches = ids[None, :, :] == expert_ids[:, None, None]
    routed = jnp.any(matches, axis=2)
    weights = jnp.sum(jnp.where(matches, gates[None, :, :], 0.0), axis=2)
    position = jnp.cumsum(routed.astype(jnp.int32), axis=1) - 1
    slot_ids = jnp.arange(CAP, dtype=jnp.int32)
    placing = (position[:, None, :] == slot_ids[None, :, None]) & routed[:, None, :]
    return matches, placing.astype(f32), weights


def own_other(pair, z):
    own = jnp.where(z == 0, pair[0], pair[1])
    other = jnp.where(z == 0, pair[1], pair[0])
    return own, other


def slot_index(z, x, y):
    gray = jnp.array(GRAY, jnp.int32)
    bits = jnp.arange(4, dtype=jnp.int32)
    xs = gray[gray[x] ^ bits]
    ys = gray[gray[y] ^ bits]
    block = xs[None, :] * 4 + ys[:, None]
    own = (z * 16 + block) * CAP
    other = ((1 - z) * 16 + block) * CAP
    none = jnp.full((4, 4, CAP), -1, jnp.int32)
    rank = jnp.arange(CAP, dtype=jnp.int32)
    return jnp.concatenate([none, own[..., None] + rank, none, other[..., None] + rank], -1)


def activate(z, pre, lane):
    fwd = (jnp.arange(ROWS) % (2 * CAP) < CAP)[:, None]
    hidden = jax.nn.silu(z[..., :F]) * z[..., F : 2 * F]
    g = pre[..., :F]
    u = pre[..., F:]
    grad_hidden = z[..., 2 * F :]
    s = jax.nn.sigmoid(g)
    activated = g * s
    dots = jnp.sum(grad_hidden * activated * u, axis=-1, keepdims=True)
    grad_gate = grad_hidden * u * s * (1.0 + g * (1.0 - s))
    grad_up = grad_hidden * activated
    h = jnp.concatenate(
        [
            jnp.where(fwd, hidden, 0.0),
            jnp.where(fwd, 0.0, grad_gate),
            jnp.where(fwd, 0.0, grad_up),
        ],
        -1,
    ).astype(bf16)
    dots = jnp.where(jnp.arange(128) == lane, jnp.where(fwd, 0.0, dots), 0.0)
    return h, dots.astype(bf16)


def project(h, w):
    out = jnp.dot(h.reshape(8 * ROWS, 3 * F), w, preferred_element_type=f32)
    return out.astype(bf16).reshape(h.shape[:-1] + (w.shape[1],))


def body(
    act_in, cotangent, fwd_ids, fwd_gates, bwd_ids, bwd_gates,
    gate_w, up_w, down_w, gate_pre, up_pre,
):
    z = lax.axis_index("z")
    x = lax.axis_index("x")
    y = lax.axis_index("y")
    matches_f, placing_f, weights_f = routing(fwd_ids[0], fwd_gates[0])
    matches_b, placing_b, weights_b = routing(bwd_ids[0], bwd_gates[0])
    own_f, other_f = own_other(placing_f, z)
    own_b, other_b = own_other(placing_b, z)
    none = jnp.zeros_like(own_f)
    pick_f = jnp.concatenate([own_f, none, other_f, none]).astype(bf16)
    pick_b = jnp.concatenate([none, own_b, none, other_b]).astype(bf16)
    rows = jnp.dot(pick_f, act_in[0], preferred_element_type=f32) + jnp.dot(
        pick_b, cotangent[0], preferred_element_type=f32
    )
    rows = rows.astype(bf16)
    swapped = lax.ppermute(rows[20:], "z", [(0, 1), (1, 0)])
    rows = jnp.concatenate([rows[:20], swapped], 0)

    scale_f = lax.ppermute(
        (placing_f * weights_f[:, None, :]).reshape(2 * CAP, TOK), "section",
        [(i, (i + 1) % 8) for i in range(8)],
    )
    scale_b = lax.ppermute(
        (placing_b * weights_b[:, None, :]).reshape(2 * CAP, TOK), "section",
        [(i, (i - 1) % 8) for i in range(8)],
    )

    got = [rows[:, s * QUARTER : (s + 1) * QUARTER].reshape(1, 1, 1, 1, ROWS, QUARTER) for s in range(4)]
    for t in range(3):
        new = [swap(got[s], (s + t) % 4) for s in range(4)]
        got = [jnp.concatenate([got[s], new[s]], 3 - (s + t) % 4) for s in range(4)]
    far = [swap(got[s], (s + 3) % 4) for s in range(4)]

    gate, up, down, got = lax.optimization_barrier((gate_w[0], up_w[0], down_w[0], got))
    w1 = jnp.concatenate([gate, up, down.T], 1)
    w2 = jnp.concatenate([down, gate.T, up.T], 0)
    pre = jnp.concatenate([gate_pre[0], up_pre[0]], 1)
    slots = jnp.arange(pre.shape[0], dtype=jnp.int32)
    pick = (slot_index(z, x, y)[..., None] == slots).astype(bf16)
    pre_rows = jnp.einsum("abrs,sf->abrf", pick, pre, preferred_element_type=f32)
    pre_rows = pre_rows.reshape(2, 2, 2, 2, ROWS, 2 * F)

    total = 0.0
    for s in range(4):
        w = w1[s * QUARTER : (s + 1) * QUARTER]
        near_z = jnp.dot(got[s].reshape(8 * ROWS, QUARTER), w, preferred_element_type=f32)
        far_z = jnp.dot(far[s].reshape(8 * ROWS, QUARTER), w, preferred_element_type=f32)
        shape = got[s].shape[:-1] + (3 * F,)
        total = total + jnp.concatenate([near_z.reshape(shape), far_z.reshape(shape)], 3 - (s + 3) % 4)
    h, dots = activate(total, pre_rows, x * 4 + y)

    keep = []
    sent = []
    for s in range(4):
        w = w2[:, s * QUARTER : (s + 1) * QUARTER]
        out = project(half(h, s, 1), w)
        if s == 3:
            out = jnp.concatenate([out, half(dots, s, 1)], -1)
        sent.append(swap(out, s))
    for s in range(4):
        w = w2[:, s * QUARTER : (s + 1) * QUARTER]
        out = project(half(h, s, 0), w)
        if s == 3:
            out = jnp.concatenate([out, half(dots, s, 0)], -1)
        keep.append(out.astype(f32))
    for t in range(1, 4):
        for s in range(4):
            d = (s + t) % 4
            keep[s] = keep[s] + sent[s].astype(f32)
            sent[s] = swap(half(keep[s], d, 1).astype(bf16), d)
            keep[s] = half(keep[s], d, 0)
    sums = [(keep[s] + sent[s].astype(f32)).reshape(ROWS, -1) for s in range(4)]
    dot_sums = jnp.sum(sums[3][:, QUARTER:], axis=1, keepdims=True)
    sums[3] = sums[3][:, :QUARTER]

    def hop(lo, step, flip):
        both = jnp.concatenate([v[lo : lo + CAP] for v in sums], 0).astype(bf16)
        pairs = []
        for s in range(8):
            for zz in range(2):
                pairs.append((s * 2 + zz, (s + step) % 8 * 2 + (zz ^ flip)))
        out = lax.ppermute(both, ("section", "z"), pairs)
        return jnp.concatenate([out[s * CAP : (s + 1) * CAP] for s in range(4)], 1)

    fo = hop(0, 1, 0)
    fx = hop(20, 1, 1)
    bo = hop(10, -1, 0)
    bx = hop(30, -1, 1)

    def place(own, other, scale):
        r = jnp.where(z == 0, jnp.concatenate([own, other], 0), jnp.concatenate([other, own], 0))
        out = jnp.einsum("rt,rd->td", scale, r.astype(f32), precision=lax.Precision.HIGHEST)
        return out.astype(bf16)[None]

    next_act = place(fo, fx, scale_f)
    prev_grad = place(bo, bx, scale_b)

    dots_own = dot_sums[10:20]
    dots_send = jnp.broadcast_to(dot_sums[30:], (CAP, 128))
    dots_other = lax.ppermute(dots_send, "z", [(0, 1), (1, 0)])[:, :1]
    dots = jnp.stack(
        [jnp.where(z == 0, dots_own, dots_other), jnp.where(z == 0, dots_other, dots_own)]
    )
    token_dots = jnp.sum(placing_b * dots, axis=1)
    gate_grad = jnp.sum(jnp.where(matches_b, token_dots[:, :, None], 0.0), axis=0)
    return next_act, prev_grad, gate_grad[None]


def solution(mesh):
    grid = Mesh(mesh.devices.reshape(8, 2, 4, 4), ("section", "z", "x", "y"))
    ex = ("z", "x", "y")
    tok = P("section", ex, None)
    col = P("section", None, ex)
    in_specs = (tok, tok, tok, tok, tok, tok, col, col, tok, col, col)
    return jax.shard_map(
        body, mesh=grid, in_specs=in_specs, out_specs=(tok, tok, tok), check_vma=False
    )
```

```python
import jax
import jax.numpy as jnp
from jax import lax
from jax.experimental import pallas as pl
from jax.experimental.pallas import tpu as pltpu
from jax.sharding import Mesh, PartitionSpec as P


CAP = 10
TOK = 128
D = 7168
F = 128
ROWS = 40
QUARTER = D // 4
SWAPS = (
    ("x", [(i, i ^ 1) for i in range(4)]),
    ("x", [(i, 3 - i) for i in range(4)]),
    ("y", [(i, i ^ 1) for i in range(4)]),
    ("y", [(i, 3 - i) for i in range(4)]),
)
GRAY = (0, 1, 3, 2)
f32 = jnp.float32
bf16 = jnp.bfloat16


def swap(v, d):
    axis, pairs = SWAPS[d]
    return lax.ppermute(v, axis, pairs)


def half(v, d, side):
    return lax.slice_in_dim(v, side, side + 1, axis=3 - d)


def routing(ids, gates):
    expert_ids = jnp.arange(2, dtype=jnp.int32)
    matches = ids[None, :, :] == expert_ids[:, None, None]
    routed = jnp.any(matches, axis=2)
    weights = jnp.sum(jnp.where(matches, gates[None, :, :], 0.0), axis=2)
    position = jnp.cumsum(routed.astype(jnp.int32), axis=1) - 1
    slot_ids = jnp.arange(CAP, dtype=jnp.int32)
    placing = (position[:, None, :] == slot_ids[None, :, None]) & routed[:, None, :]
    return matches, placing.astype(f32), weights


def own_other(pair, z):
    own = jnp.where(z == 0, pair[0], pair[1])
    other = jnp.where(z == 0, pair[1], pair[0])
    return own, other


def slot_index(z, x, y):
    gray = jnp.array(GRAY, jnp.int32)
    bits = jnp.arange(4, dtype=jnp.int32)
    xs = gray[gray[x] ^ bits]
    ys = gray[gray[y] ^ bits]
    block = xs[None, :] * 4 + ys[:, None]
    own = (z * 16 + block) * CAP
    other = ((1 - z) * 16 + block) * CAP
    none = jnp.full((4, 4, CAP), -1, jnp.int32)
    rank = jnp.arange(CAP, dtype=jnp.int32)
    return jnp.concatenate([none, own[..., None] + rank, none, other[..., None] + rank], -1)


def turn_kernel(down, after, out):
    del after
    out[...] = down[...].T


def turned(down, after):
    return pl.pallas_call(
        turn_kernel,
        grid=(8,),
        in_specs=[
            pl.BlockSpec((F, D // 8), lambda s: (0, s)),
            pl.BlockSpec((8, 128), lambda s: (0, 0)),
        ],
        out_specs=pl.BlockSpec((D // 8, F), lambda s: (s, 0)),
        out_shape=jax.ShapeDtypeStruct((D, F), bf16),
        compiler_params=pltpu.CompilerParams(vmem_limit_bytes=4 * 2**20),
    )(down, after)


def activate(z, pre, lane):
    fwd = (jnp.arange(ROWS) % (2 * CAP) < CAP)[:, None]
    hidden = jax.nn.silu(z[..., :F]) * z[..., F : 2 * F]
    g = pre[..., :F]
    u = pre[..., F:]
    grad_hidden = z[..., 2 * F :]
    s = jax.nn.sigmoid(g)
    activated = g * s
    dots = jnp.sum(grad_hidden * activated * u, axis=-1, keepdims=True)
    grad_gate = grad_hidden * u * s * (1.0 + g * (1.0 - s))
    grad_up = grad_hidden * activated
    h = jnp.concatenate(
        [
            jnp.where(fwd, 0.0, grad_gate),
            jnp.where(fwd, 0.0, grad_up),
            jnp.where(fwd, hidden, 0.0),
        ],
        -1,
    ).astype(bf16)
    dots = jnp.where(jnp.arange(128) == lane, jnp.where(fwd, 0.0, dots), 0.0)
    return h, dots.astype(bf16)


def project(h, w):
    out = lax.dot_general(
        h.reshape(8 * ROWS, 3 * F), w, (((1,), (1,)), ((), ())), preferred_element_type=f32
    )
    return out.astype(bf16).reshape(h.shape[:-1] + (QUARTER,))


def pieces(scale):
    high = lax.reduce_precision(scale, 8, 7)
    rest = scale - high
    mid = lax.reduce_precision(rest, 8, 7)
    low = lax.reduce_precision(rest - mid, 8, 7)
    return jnp.concatenate([high, mid, low], 0).astype(bf16)


def body(
    act_in, cotangent, fwd_ids, fwd_gates, bwd_ids, bwd_gates,
    gate_w, up_w, down_w, gate_pre, up_pre,
):
    z = lax.axis_index("z")
    x = lax.axis_index("x")
    y = lax.axis_index("y")
    _, placing_f, weights_f = routing(fwd_ids[0], fwd_gates[0])
    _, placing_b, weights_b = routing(bwd_ids[0], bwd_gates[0])
    own_f, other_f = own_other(placing_f, z)
    own_b, other_b = own_other(placing_b, z)
    none = jnp.zeros_like(own_f)

    def collect(f, b):
        left = jnp.concatenate([f, none]).astype(bf16)
        right = jnp.concatenate([none, b]).astype(bf16)
        both = jnp.dot(left, act_in[0], preferred_element_type=f32) + jnp.dot(
            right, cotangent[0], preferred_element_type=f32
        )
        return both.astype(bf16)

    swapped = lax.ppermute(collect(other_f, other_b), "z", [(0, 1), (1, 0)])
    rows = jnp.concatenate([collect(own_f, own_b), swapped], 0)

    got = [rows[:, s * QUARTER : (s + 1) * QUARTER].reshape(1, 1, 1, 1, ROWS, QUARTER) for s in range(4)]
    for t in range(3):
        new = [swap(got[s], (s + t) % 4) for s in range(4)]
        got = [jnp.concatenate([got[s], new[s]], 3 - (s + t) % 4) for s in range(4)]
    far = [swap(got[s], (s + 3) % 4) for s in range(4)]

    after = got[3].reshape(-1, QUARTER)[:8, :128]
    down_t = turned(down_w[0], after)
    w = jnp.concatenate([gate_w[0], up_w[0], down_t], 1)
    w = [w[s * QUARTER : (s + 1) * QUARTER] for s in range(4)]
    flat = lambda p, v: (p * v[:, None, :]).reshape(2 * CAP, TOK)
    ahead = [(i, (i + 1) % 8) for i in range(8)]
    back = [(i, (i - 1) % 8) for i in range(8)]
    scale_f = pieces(lax.ppermute(flat(placing_f, weights_f), "section", ahead))
    scale_b = pieces(lax.ppermute(flat(placing_b, weights_b), "section", back))
    pre = jnp.concatenate([gate_pre[0], up_pre[0]], 1)
    slots = jnp.arange(pre.shape[0], dtype=jnp.int32)
    pick = (slot_index(z, x, y)[..., None] == slots).astype(bf16).reshape(16 * ROWS, -1)
    pre_rows = jnp.dot(pick, pre, preferred_element_type=f32)
    pre_rows = pre_rows.reshape(2, 2, 2, 2, ROWS, 2 * F)

    total = 0.0
    for s in range(4):
        near_z = jnp.dot(got[s].reshape(8 * ROWS, QUARTER), w[s], preferred_element_type=f32)
        far_z = jnp.dot(far[s].reshape(8 * ROWS, QUARTER), w[s], preferred_element_type=f32)
        shape = got[s].shape[:-1] + (3 * F,)
        total = total + jnp.concatenate([near_z.reshape(shape), far_z.reshape(shape)], 3 - (s + 3) % 4)
    h, dots = activate(total, pre_rows, x * 4 + y)

    def partial(s, side):
        out = project(half(h, s, side), w[s])
        return jnp.concatenate([out, half(dots, s, side)], -1) if s == 3 else out

    sent = [swap(partial(s, 1), s) for s in range(4)]
    keep = [partial(s, 0).astype(f32) for s in range(4)]
    for t in range(1, 4):
        for s in range(4):
            d = (s + t) % 4
            keep[s] = keep[s] + sent[s].astype(f32)
            sent[s] = swap(half(keep[s], d, 1).astype(bf16), d)
            keep[s] = half(keep[s], d, 0)
    sums = [(keep[s] + sent[s].astype(f32)).reshape(ROWS, -1) for s in range(4)]
    row_dots = jnp.sum(sums[3][:, QUARTER:], axis=1, keepdims=True)
    sums[3] = sums[3][:, :QUARTER]

    def hop(lo, step, flip):
        both = jnp.concatenate([v[lo : lo + CAP].astype(bf16) for v in sums], 0)
        pairs = []
        for s in range(8):
            for zz in range(2):
                pairs.append((s * 2 + zz, (s + step) % 8 * 2 + (zz ^ flip)))
        out = lax.ppermute(both, ("section", "z"), pairs)
        return jnp.concatenate([out[s * CAP : (s + 1) * CAP] for s in range(4)], 1)

    fo = hop(0, 1, 0)
    fx = hop(20, 1, 1)
    bo = hop(10, -1, 0)
    bx = hop(30, -1, 1)

    def place(own, other, scale):
        r = jnp.where(z == 0, jnp.concatenate([own, other], 0), jnp.concatenate([other, own], 0))
        out = lax.dot_general(
            scale, jnp.concatenate([r, r, r], 0), (((0,), (0,)), ((), ())),
            preferred_element_type=f32,
        )
        return out.astype(bf16)[None]

    next_act = place(fo, fx, scale_f)
    prev_grad = place(bo, bx, scale_b)

    dots_own = row_dots[10:20]
    dots_send = jnp.broadcast_to(row_dots[30:], (CAP, 128))
    dots_other = lax.ppermute(dots_send, "z", [(0, 1), (1, 0)])[:, :1]
    dot_sums = jnp.stack(
        [jnp.where(z == 0, dots_own, dots_other), jnp.where(z == 0, dots_other, dots_own)]
    )
    dot_sums, late_ids = lax.optimization_barrier((dot_sums, bwd_ids[0]))
    matches_late = late_ids[None, :, :] == jnp.arange(2, dtype=jnp.int32)[:, None, None]
    token_dots = jnp.sum(placing_b * dot_sums, axis=1)
    gate_grad = jnp.sum(jnp.where(matches_late, token_dots[:, :, None], 0.0), axis=0)
    return next_act, prev_grad, gate_grad[None]


def solution(mesh):
    grid = Mesh(mesh.devices.reshape(8, 2, 4, 4), ("section", "z", "x", "y"))
    ex = ("z", "x", "y")
    tok = P("section", ex, None)
    col = P("section", None, ex)
    in_specs = (tok, tok, tok, tok, tok, tok, col, col, tok, col, col)
    return jax.shard_map(
        body, mesh=grid, in_specs=in_specs, out_specs=(tok, tok, tok), check_vma=False
    )
```

```python
import jax
import jax.numpy as jnp
from jax import lax
from jax.experimental import pallas as pl
from jax.experimental.pallas import tpu as pltpu
from jax.sharding import Mesh, PartitionSpec as P


CAP = 10
TOK = 128
D = 7168
F = 128
ROWS = 40
QUARTER = D // 4
SWAPS = (
    ("x", [(i, i ^ 1) for i in range(4)]),
    ("x", [(i, 3 - i) for i in range(4)]),
    ("y", [(i, i ^ 1) for i in range(4)]),
    ("y", [(i, 3 - i) for i in range(4)]),
)
GRAY = (0, 1, 3, 2)
f32 = jnp.float32
bf16 = jnp.bfloat16


def swap(v, d):
    axis, pairs = SWAPS[d]
    return lax.ppermute(v, axis, pairs)


def half(v, d, side):
    return lax.slice_in_dim(v, side, side + 1, axis=3 - d)


def routing(ids, gates):
    expert_ids = jnp.arange(2, dtype=jnp.int32)
    matches = ids[None, :, :] == expert_ids[:, None, None]
    routed = jnp.any(matches, axis=2)
    weights = jnp.sum(jnp.where(matches, gates[None, :, :], 0.0), axis=2)
    position = jnp.cumsum(routed.astype(jnp.int32), axis=1) - 1
    slot_ids = jnp.arange(CAP, dtype=jnp.int32)
    placing = (position[:, None, :] == slot_ids[None, :, None]) & routed[:, None, :]
    return matches, placing.astype(f32), weights


def own_other(pair, z):
    own = jnp.where(z == 0, pair[0], pair[1])
    other = jnp.where(z == 0, pair[1], pair[0])
    return own, other


def slot_index(z, x, y):
    gray = jnp.array(GRAY, jnp.int32)
    bits = jnp.arange(4, dtype=jnp.int32)
    xs = gray[gray[x] ^ bits]
    ys = gray[gray[y] ^ bits]
    block = xs[None, :] * 4 + ys[:, None]
    own = (z * 16 + block) * CAP
    other = ((1 - z) * 16 + block) * CAP
    none = jnp.full((4, 4, CAP), -1, jnp.int32)
    rank = jnp.arange(CAP, dtype=jnp.int32)
    return jnp.concatenate([none, own[..., None] + rank, none, other[..., None] + rank], -1)


def turn_kernel(down, after, out):
    del after
    out[...] = down[...].T


def turned(down, after):
    return pl.pallas_call(
        turn_kernel,
        grid=(8,),
        in_specs=[
            pl.BlockSpec((F, D // 8), lambda s: (0, s)),
            pl.BlockSpec((8, 128), lambda s: (0, 0)),
        ],
        out_specs=pl.BlockSpec((D // 8, F), lambda s: (s, 0)),
        out_shape=jax.ShapeDtypeStruct((D, F), bf16),
        compiler_params=pltpu.CompilerParams(vmem_limit_bytes=4 * 2**20),
    )(down, after)


def activate(z, pre, lane):
    fwd = (jnp.arange(ROWS) % (2 * CAP) < CAP)[:, None]
    hidden = jax.nn.silu(z[..., :F]) * z[..., F : 2 * F]
    g = pre[..., :F]
    u = pre[..., F:]
    grad_hidden = z[..., 2 * F :]
    s = jax.nn.sigmoid(g)
    activated = g * s
    dots = jnp.sum(grad_hidden * activated * u, axis=-1, keepdims=True)
    grad_gate = grad_hidden * u * s * (1.0 + g * (1.0 - s))
    grad_up = grad_hidden * activated
    h = jnp.concatenate(
        [
            jnp.where(fwd, 0.0, grad_gate),
            jnp.where(fwd, 0.0, grad_up),
            jnp.where(fwd, hidden, 0.0),
        ],
        -1,
    ).astype(bf16)
    dots = jnp.where(jnp.arange(128) == lane, jnp.where(fwd, 0.0, dots), 0.0)
    return h, dots.astype(bf16)


def project(h, w):
    out = lax.dot_general(
        h.reshape(8 * ROWS, 3 * F), w, (((1,), (1,)), ((), ())), preferred_element_type=f32
    )
    return out.astype(bf16).reshape(h.shape[:-1] + (QUARTER,))


def pieces(scale):
    high = lax.reduce_precision(scale, 8, 7)
    rest = scale - high
    mid = lax.reduce_precision(rest, 8, 7)
    low = lax.reduce_precision(rest - mid, 8, 7)
    return jnp.concatenate([high, mid, low], 0).astype(bf16)


def body(
    act_in, cotangent, fwd_ids, fwd_gates, bwd_ids, bwd_gates,
    gate_w, up_w, down_w, gate_pre, up_pre,
):
    z = lax.axis_index("z")
    x = lax.axis_index("x")
    y = lax.axis_index("y")
    _, placing_f, weights_f = routing(fwd_ids[0], fwd_gates[0])
    _, placing_b, weights_b = routing(bwd_ids[0], bwd_gates[0])
    own_f, other_f = own_other(placing_f, z)
    own_b, other_b = own_other(placing_b, z)
    none = jnp.zeros_like(own_f)

    def collect(f, b):
        left = jnp.concatenate([f, none]).astype(bf16)
        right = jnp.concatenate([none, b]).astype(bf16)
        both = jnp.dot(left, act_in[0], preferred_element_type=f32) + jnp.dot(
            right, cotangent[0], preferred_element_type=f32
        )
        return both.astype(bf16)

    away = collect(other_f, other_b)
    own = collect(own_f, own_b)
    both = []
    for k in range(2):
        side = slice(k * D // 2, (k + 1) * D // 2)
        swapped = lax.ppermute(away[:, side], "z", [(0, 1), (1, 0)])
        both.append(jnp.concatenate([own[:, side], swapped], 0))

    got = [
        both[s // 2][:, s % 2 * QUARTER : (s % 2 + 1) * QUARTER].reshape(1, 1, 1, 1, ROWS, QUARTER)
        for s in range(4)
    ]
    for t in range(3):
        new = [swap(got[s], (s + t) % 4) for s in range(4)]
        got = [jnp.concatenate([got[s], new[s]], 3 - (s + t) % 4) for s in range(4)]
    far = [swap(got[s], (s + 3) % 4) for s in range(4)]

    after = got[3].reshape(-1, QUARTER)[:8, :128]
    down_t = turned(down_w[0], after)
    w = jnp.concatenate([gate_w[0], up_w[0], down_t], 1)
    w = [w[s * QUARTER : (s + 1) * QUARTER] for s in range(4)]
    flat = lambda p, v: (p * v[:, None, :]).reshape(2 * CAP, TOK)
    ahead = [(i, (i + 1) % 8) for i in range(8)]
    back = [(i, (i - 1) % 8) for i in range(8)]
    scale_f = pieces(lax.ppermute(flat(placing_f, weights_f), "section", ahead))
    scale_b = pieces(lax.ppermute(flat(placing_b, weights_b), "section", back))
    pre = jnp.concatenate([gate_pre[0], up_pre[0]], 1)
    slots = jnp.arange(pre.shape[0], dtype=jnp.int32)
    pick = (slot_index(z, x, y)[..., None] == slots).astype(bf16).reshape(16 * ROWS, -1)
    pre_rows = jnp.dot(pick, pre, preferred_element_type=f32)
    pre_rows = pre_rows.reshape(2, 2, 2, 2, ROWS, 2 * F)

    total = 0.0
    for s in range(4):
        near_z = jnp.dot(got[s].reshape(8 * ROWS, QUARTER), w[s], preferred_element_type=f32)
        far_z = jnp.dot(far[s].reshape(8 * ROWS, QUARTER), w[s], preferred_element_type=f32)
        shape = got[s].shape[:-1] + (3 * F,)
        total = total + jnp.concatenate([near_z.reshape(shape), far_z.reshape(shape)], 3 - (s + 3) % 4)
    h, dots = activate(total, pre_rows, x * 4 + y)

    def partial(s, side):
        out = project(half(h, s, side), w[s])
        return jnp.concatenate([out, half(dots, s, side)], -1) if s == 3 else out

    sent = [swap(partial(s, 1), s) for s in range(4)]
    keep = [partial(s, 0).astype(f32) for s in range(4)]
    for t in range(1, 4):
        for s in range(4):
            d = (s + t) % 4
            keep[s] = keep[s] + sent[s].astype(f32)
            sent[s] = swap(half(keep[s], d, 1).astype(bf16), d)
            keep[s] = half(keep[s], d, 0)
    sums = [(keep[s] + sent[s].astype(f32)).reshape(ROWS, -1) for s in range(4)]
    row_dots = jnp.sum(sums[3][:, QUARTER:], axis=1, keepdims=True)
    sums[3] = sums[3][:, :QUARTER]

    def hop(lo, step, flip):
        both = jnp.concatenate([v[lo : lo + CAP].astype(bf16) for v in sums], 0)
        pairs = []
        for s in range(8):
            for zz in range(2):
                pairs.append((s * 2 + zz, (s + step) % 8 * 2 + (zz ^ flip)))
        out = lax.ppermute(both, ("section", "z"), pairs)
        return jnp.concatenate([out[s * CAP : (s + 1) * CAP] for s in range(4)], 1)

    fo = hop(0, 1, 0)
    fx = hop(20, 1, 1)
    bo = hop(10, -1, 0)
    bx = hop(30, -1, 1)

    def place(own, other, scale):
        r = jnp.where(z == 0, jnp.concatenate([own, other], 0), jnp.concatenate([other, own], 0))
        out = lax.dot_general(
            scale, jnp.concatenate([r, r, r], 0), (((0,), (0,)), ((), ())),
            preferred_element_type=f32,
        )
        return out.astype(bf16)[None]

    next_act = place(fo, fx, scale_f)
    prev_grad = place(bo, bx, scale_b)

    dots_own = row_dots[10:20]
    dots_send = jnp.broadcast_to(row_dots[30:], (CAP, 128))
    dots_other = lax.ppermute(dots_send, "z", [(0, 1), (1, 0)])[:, :1]
    dot_sums = jnp.stack(
        [jnp.where(z == 0, dots_own, dots_other), jnp.where(z == 0, dots_other, dots_own)]
    )
    dot_sums, late_ids = lax.optimization_barrier((dot_sums, bwd_ids[0]))
    matches_late = late_ids[None, :, :] == jnp.arange(2, dtype=jnp.int32)[:, None, None]
    token_dots = jnp.sum(placing_b * dot_sums, axis=1)
    gate_grad = jnp.sum(jnp.where(matches_late, token_dots[:, :, None], 0.0), axis=0)
    return next_act, prev_grad, gate_grad[None]


def solution(mesh):
    grid = Mesh(mesh.devices.reshape(8, 2, 4, 4), ("section", "z", "x", "y"))
    ex = ("z", "x", "y")
    tok = P("section", ex, None)
    col = P("section", None, ex)
    in_specs = (tok, tok, tok, tok, tok, tok, col, col, tok, col, col)
    return jax.shard_map(
        body, mesh=grid, in_specs=in_specs, out_specs=(tok, tok, tok), check_vma=False
    )
```
